32 devices in a mesh: mode: 8 (over z, y), cores: 4 (over x, core).
Axes of the slice: x: 2, y: 2, z: 4, core: 2. Of those that a mesh axis runs over, the one named last changes fastest.
Arguments:
- train_cores: bfloat16 [4, 400, 32, 400], P('cores', None, 'mode'), may hold values from -0.24748737 to 0.24748737
- sketch_cores: bfloat16 [4, 100, 32, 100], P('cores', None, 'mode'), may hold values from -0.3125 to 0.3125
- left_interface: float32 [100, 400], replicated, may hold values from -6 to 6
- right_sketch: bfloat16 [400, 100], replicated, may hold values from -6 to 6
Outputs:
- frames: bfloat16 [4, 100, 32, 100], P('cores', None, 'mode')
- interfaces: float32 [4, 100, 400], P('cores')
The draws below stay inside these ranges and needn't reach their ends.
All inputs are finite; a program needn't handle non-finite values.
Results may differ from the reference program's by a relative error of at most 0.019.
Values may be sent and summed in bfloat16 or wider, within the bound.
A program may use at most 64 MiB of HBM per device.

```python
import math
import jax
import jax.numpy as jnp
from jax import lax

RANK = 400
SKETCH = 100
MODE = 32
CHAIN = 4


def draw_train_cores(key, part):
    key_scale = jax.random.fold_in(key, 11)
    key_entry = jax.random.fold_in(key, 12)
    exponent = jax.random.uniform(key_scale, (CHAIN, 1, MODE, 1), jnp.float32)
    factor = jnp.exp(exponent * math.log(10.0)) / 4.6
    entries = jnp.clip(jax.random.normal(key_entry, (CHAIN, RANK, MODE, RANK), jnp.float32), -6.0, 6.0)
    return (entries * factor / math.sqrt(MODE * SKETCH)).astype(jnp.bfloat16)


def levels(key, dims, cuts, smallest, largest):
    gain, own = 1.0, jax.random.fold_in(key, 6)
    for position, parts in cuts:
        heights = jnp.exp(jax.random.uniform(jax.random.fold_in(own, position), (parts,), jnp.float32, smallest / len(cuts), largest / len(cuts)))
        gain = gain * jnp.repeat(heights, dims[position] // parts).reshape([-1 if axis == position else 1 for axis in range(len(dims))])
    return gain


def gaussian(stream_key, shape, deviation, limit, shards=(), kind=jnp.bfloat16):
    values = deviation * jax.random.normal(stream_key, shape, jnp.float32)
    if shards:
        values = values * levels(stream_key, shape, shards, -0.22, 0.18)
    return jnp.clip(values, -limit, limit).astype(kind)


def setup_inputs(seed: int = 0) -> dict:
    keys = jax.random.split(jax.random.key(seed), 5)
    return {
        "train_cores": draw_train_cores(jax.random.fold_in(keys[4], 71), 0),
        "sketch_cores": gaussian(keys[1], (CHAIN, SKETCH, MODE, SKETCH), RANK ** -0.5, 0.3125, ((0, 4), (2, 8))),
        "left_interface": gaussian(keys[2], (SKETCH, RANK), 1.0, 6.0, (), jnp.float32),
        "right_sketch": gaussian(keys[3], (RANK, SKETCH), 1.0, 6.0),
    }


def reference(train_cores, sketch_cores, left_interface, right_sketch):
    sketches = [right_sketch]
    for index in range(CHAIN - 1, 0, -1):
        flat_core = train_cores[index].reshape(RANK * MODE, RANK)
        partial_value = jnp.dot(flat_core.astype(jnp.float32), sketches[0].astype(jnp.float32), preferred_element_type=jnp.float32).astype(jnp.bfloat16)
        partial_value = partial_value.reshape(RANK, MODE * SKETCH)
        sketch_flat = sketch_cores[index].reshape(SKETCH, MODE * SKETCH)
        next_sketch = lax.dot_general(partial_value.astype(jnp.float32), sketch_flat.astype(jnp.float32), (((1,), (1,)), ((), ())), preferred_element_type=jnp.float32)
        sketches.insert(0, next_sketch.astype(jnp.bfloat16))
    frame_scale = math.sqrt(SKETCH * MODE)
    carry = left_interface
    frame_list = []
    carry_list = []
    for index in range(CHAIN):
        carry_low = carry.astype(jnp.bfloat16)
        built = jnp.dot(carry_low.astype(jnp.float32), train_cores[index].reshape(RANK, MODE * RANK).astype(jnp.float32), preferred_element_type=jnp.float32)
        built = built.astype(jnp.bfloat16).reshape(SKETCH * MODE, RANK)
        images = jnp.dot(built.astype(jnp.float32), sketches[index].astype(jnp.float32), preferred_element_type=jnp.float32)
        gram_matrix = lax.dot_general(images, images, (((0,), (0,)), ((), ())), precision=lax.Precision.HIGHEST)
        chol_lower = jnp.linalg.cholesky(gram_matrix)
        frame_rows = lax.linalg.triangular_solve(chol_lower, images.T, left_side=True, lower=True)
        frame_list.append((frame_rows.T * frame_scale).astype(jnp.bfloat16).reshape(SKETCH, MODE, SKETCH))
        carry = jnp.dot(frame_rows, built.astype(jnp.float32), precision=lax.Precision.HIGHEST)
        carry_list.append(carry)
    return (jnp.stack(frame_list), jnp.stack(carry_list))
```

```python
import functools
import math

import jax
import jax.numpy as jnp
from jax import lax
from jax.experimental import pallas as pl
from jax.experimental.pallas import tpu as pltpu
from jax.sharding import PartitionSpec as P

MESH = pl.DeviceIdType.MESH
F32, BF16 = jnp.float32, jnp.bfloat16
EXACT = lax.Precision.HIGHEST


def up(value, step):
    return -(-value // step) * step


def dot(a, b, ca, cb, precision=None):
    return lax.dot_general(
        a, b, (((ca,), (cb,)), ((), ())), preferred_element_type=F32, precision=precision
    )


def when(condition, run):
    if condition is True:
        run()
    else:
        pl.when(condition)(run)


def lower_inverse(gram, size, look=4):
    full = gram.shape[0]
    lane = lax.broadcasted_iota(jnp.int32, (1, full), 1)
    top, table, done = 0, gram, []
    for first in range(0, size, look):
        base = first // 8 * 8
        if base > top:
            done.append(table[: base - top])
            table = table[base - top :]
            top = base
        rows = full - top
        width = min(look, size - first)
        row_id = lax.broadcasted_iota(jnp.int32, (rows, full), 0) + top
        columns = [
            jnp.broadcast_to(table[:, first + t : first + t + 1], (rows, full)) for t in range(width)
        ]
        for t in range(width):
            j = first + t
            here = j - top
            column = columns[t]
            pivot = column[here : here + 1]
            inverse = 1.0 / pivot
            row = jnp.where(lane == j, 1.0, table[here : here + 1]) * inverse
            below = row_id > j
            lower = jnp.where(below, column, 0.0)
            for s in range(t + 1, width):
                ahead = here + s - t
                columns[s] = columns[s] - lower * (column[ahead : ahead + 1] * inverse)
            table = jnp.where((lane == j) & below, 0.0, table) - lower * row
    done.append(table)
    table = jnp.concatenate(done, axis=0) if len(done) > 1 else table
    row_id = lax.broadcasted_iota(jnp.int32, (full, full), 0)
    lane = lax.broadcasted_iota(jnp.int32, (full, full), 1)
    pivots = jnp.sum(jnp.where(row_id == lane, table, 0.0), axis=1, keepdims=True)
    unit = jnp.where(row_id > lane, table, jnp.where(row_id == lane, 1.0, 0.0))
    return unit * lax.rsqrt(pivots)


def kernel(
    dims,
    core_ref,
    gauss_ref,
    left_ref,
    right_ref,
    frames_ref,
    faces_ref,
    sketch_buf,
    part_out,
    part_in,
    carry_buf,
    carry_own,
    proj_out,
    proj_in,
    gram_out,
    gram_in,
    piece_sk,
    piece_ca,
    s_part,
    r_part,
    s_sk,
    r_sk,
    s_proj,
    r_proj,
    s_gram,
    r_gram,
    s_next,
    r_next,
    s_own,
    r_own,
):
    size, group_count, rank, sketch, modes, chunk, owners, scale = dims
    rank_pad, sketch_pad = owners * chunk, gauss_ref.shape[1]
    me = lax.axis_index("mode")
    group = lax.axis_index("cores")
    final = group_count - 1
    owner = True if owners == size else me < owners

    def scatter(out_ref, in_ref, sends, recvs, target=None):
        copies = []
        for d in range(1, size):
            peer = lax.rem(me + d, size)
            copies.append(
                pltpu.make_async_remote_copy(
                    src_ref=out_ref.at[peer] if target is None else out_ref,
                    dst_ref=in_ref.at[d],
                    send_sem=sends.at[d],
                    recv_sem=recvs.at[d],
                    device_id={"mode": peer},
                    device_id_type=MESH,
                )
            )
        return copies

    def chunk_sends(copies, act):
        for d, copy in enumerate(copies, 1):
            peer = lax.rem(me + d, size)
            when(True if owners == size else peer < owners, functools.partial(act, copy))

    def spread(piece_ref, buf_ref, sends, recvs, to_group, skip_self):
        copies = []
        for d in range(1 if skip_self else 0, size):
            peer = lax.rem(me + d, size)
            copies.append(
                pltpu.make_async_remote_copy(
                    src_ref=piece_ref,
                    dst_ref=buf_ref.at[me],
                    send_sem=sends.at[d],
                    recv_sem=recvs.at[me],
                    device_id={"mode": peer, "cores": to_group},
                    device_id_type=MESH,
                )
            )
        return copies

    def await_chunk(buf_ref, recvs, source):
        pltpu.make_async_remote_copy(
            src_ref=buf_ref.at[source],
            dst_ref=buf_ref.at[source],
            send_sem=recvs.at[source],
            recv_sem=recvs.at[source],
            device_id={"mode": lax.rem(me + 1, size)},
            device_id_type=MESH,
        ).wait_recv()

    @pl.when(group == final)
    def _():
        sketch_buf[...] = right_ref[...].reshape(sketch_buf.shape)

    @pl.when(group < final)
    def _():
        for source in range(owners):
            await_chunk(sketch_buf, r_sk, source)

    down = lax.rem(group + group_count - 1, group_count)
    upward = lax.rem(group + 1, group_count)
    part_copies = scatter(part_out, part_in, s_part, r_part)
    sk_copies = spread(piece_sk, sketch_buf, s_sk, r_sk, down, False)

    @pl.when(group > 0)
    def _():
        held = sketch_buf[...].reshape(rank_pad, sketch_pad)
        total = None
        for i in range(modes):
            partial_value = dot(core_ref[i], held, 1, 0).astype(BF16)
            term = dot(partial_value, gauss_ref[i], 1, 1)
            total = term if total is None else total + term
        part_out[...] = total.astype(part_out.dtype).reshape(part_out.shape)
        chunk_sends(part_copies, lambda c: c.start())

        def finish():
            value = part_out[me].astype(F32)
            for d in range(1, size):
                part_copies[d - 1].wait_recv()
                value = value + part_in[d].astype(F32)
            piece_sk[...] = value.astype(BF16)
            for copy in sk_copies:
                copy.start()
            for copy in sk_copies:
                copy.wait_send()

        when(owner, finish)
        chunk_sends(part_copies, lambda c: c.wait_send())

    @pl.when(group == 0)
    def _():
        carry_buf[...] = left_ref[...].reshape(carry_buf.shape)

    @pl.when(group > 0)
    def _():
        for source in range(owners):
            await_chunk(carry_buf, r_next, source)

    carry = carry_buf[...].reshape(rank_pad, sketch_pad)
    held = sketch_buf[...].reshape(rank_pad, sketch_pad)
    gram_copies = scatter(gram_out, gram_in, s_gram, r_gram, True)
    proj_copies = scatter(proj_out, proj_in, s_proj, r_proj)
    images, halves, builts = [], [], []
    gram = None
    for i in range(modes):
        built = dot(carry, core_ref[i], 0, 0).astype(BF16)
        image = dot(built, held, 1, 0)
        high = image.astype(BF16)
        low = (image - high.astype(F32)).astype(BF16)
        cross = dot(high, low, 0, 0)
        term = dot(high, high, 0, 0) + dot(low, high, 0, 0) + cross
        gram = term if gram is None else gram + term
        images.append(image)
        halves.append((high, low))
        builts.append(built)
    gram_rows = gram_out.shape[0]
    gram_out[...] = gram[:gram_rows]
    for copy in gram_copies:
        copy.start()
    proj = None
    for (high, low), built in zip(halves, builts):
        term = dot(built, high, 0, 0) + dot(built, low, 0, 0)
        proj = term if proj is None else proj + term
    proj_out[...] = proj.astype(proj_out.dtype).reshape(proj_out.shape)
    chunk_sends(proj_copies, lambda c: c.start())

    for copy in gram_copies:
        copy.wait_recv()
    gram_in[0] = gram_out[...]
    total = None
    for source in range(size):
        term = gram_in[lax.rem(me - source + size, size)]
        total = term if total is None else total + term
    if gram_rows < sketch_pad:
        total = jnp.concatenate([total, jnp.zeros((sketch_pad - gram_rows, sketch_pad), F32)], 0)
    row_id = lax.broadcasted_iota(jnp.int32, (sketch_pad, sketch_pad), 0)
    lane_id = lax.broadcasted_iota(jnp.int32, (sketch_pad, sketch_pad), 1)
    total = jnp.where((row_id == lane_id) & (row_id >= sketch), 1.0, total)
    inverse = lower_inverse(total, sketch)

    next_copies = spread(piece_ca, carry_buf, s_next, r_next, upward, False)
    own_copies = spread(piece_ca, carry_own, s_own, r_own, group, True)

    def project():
        value = proj_out[me].astype(F32)
        for d in range(1, size):
            proj_copies[d - 1].wait_recv()
            value = value + proj_in[d].astype(F32)
        piece_ca[...] = dot(value, inverse, 1, 1, EXACT).astype(BF16)

        @pl.when(group < final)
        def _():
            for copy in next_copies:
                copy.start()

        for copy in own_copies:
            copy.start()
        carry_own[me] = piece_ca[...]

    when(owner, project)
    for i in range(modes):
        orth = dot(images[i], inverse, 1, 1, EXACT)
        frames_ref[i] = (orth * scale).astype(BF16)
    chunk_sends(proj_copies, lambda c: c.wait_send())
    for copy in gram_copies:
        copy.wait_send()
    for source in range(owners):

        @pl.when(me != source)
        def _(source=source):
            await_chunk(carry_own, r_own, source)

    faces = carry_own[...].reshape(rank_pad, sketch_pad).astype(F32).T
    faces_ref[...] = faces

    def drain():
        for copy in own_copies:
            copy.wait_send()

        @pl.when(group < final)
        def _():
            for copy in next_copies:
                copy.wait_send()

    when(owner, drain)


def body(train_cores, sketch_cores, left_interface, right_sketch):
    size = lax.axis_size("mode")
    group_count = lax.axis_size("cores")
    _, rank, modes, _ = train_cores.shape
    sketch = sketch_cores.shape[1]
    sketch_pad = up(sketch, 128)
    chunk = up(-(-up(rank, 128) // size), 16)
    owners = -(-rank // chunk)
    chunk_total = owners * chunk
    rank_pad = up(chunk_total, 128)
    owners = rank_pad // chunk if rank_pad % chunk == 0 else owners
    rank_pad = owners * chunk
    core = jnp.pad(
        train_cores[0].transpose(1, 0, 2), ((0, 0), (0, rank_pad - rank), (0, rank_pad - rank))
    )
    gauss = jnp.pad(
        sketch_cores[0].transpose(1, 0, 2),
        ((0, 0), (0, sketch_pad - sketch), (0, sketch_pad - sketch)),
    )
    left = jnp.pad(
        left_interface.astype(BF16).T, ((0, rank_pad - rank), (0, sketch_pad - sketch))
    )
    right = jnp.pad(right_sketch, ((0, rank_pad - rank), (0, sketch_pad - sketch)))
    scale = math.sqrt(sketch * modes * size)
    dims = (size, group_count, rank, sketch, modes, chunk, owners, scale)
    gram_rows = up(sketch, 8)
    chunks = (owners, chunk, sketch_pad)
    vmem = pl.BlockSpec(memory_space=pltpu.VMEM)
    dma = pltpu.SemaphoreType.DMA((size,))
    frames, faces = pl.pallas_call(
        functools.partial(kernel, dims),
        out_shape=(
            jax.ShapeDtypeStruct((modes, sketch_pad, sketch_pad), BF16),
            jax.ShapeDtypeStruct((sketch_pad, rank_pad), F32),
        ),
        in_specs=[vmem] * 4,
        out_specs=(vmem, vmem),
        scratch_shapes=[
            pltpu.VMEM(chunks, BF16),
            pltpu.VMEM(chunks, F32),
            pltpu.VMEM((size, chunk, sketch_pad), F32),
            pltpu.VMEM(chunks, BF16),
            pltpu.VMEM(chunks, BF16),
            pltpu.VMEM(chunks, F32),
            pltpu.VMEM((size, chunk, sketch_pad), F32),
            pltpu.VMEM((gram_rows, sketch_pad), F32),
            pltpu.VMEM((size, gram_rows, sketch_pad), F32),
            pltpu.VMEM((chunk, sketch_pad), BF16),
            pltpu.VMEM((chunk, sketch_pad), BF16),
        ]
        + [dma] * 12,
        compiler_params=pltpu.CompilerParams(has_side_effects=True),
    )(core, gauss, left, right)
    frames = frames[:, :sketch, :sketch].transpose(1, 0, 2)[None]
    return frames, faces[None, :sketch, :rank]


def solution(mesh):
    in_specs = (P("cores", None, "mode", None), P("cores", None, "mode", None), P(), P())
    out_specs = (P("cores", None, "mode", None), P("cores", None, None))
    return jax.shard_map(body, mesh=mesh, in_specs=in_specs, out_specs=out_specs, check_vma=False)
```

```python
import functools
import math

import jax
import jax.numpy as jnp
from jax import lax
from jax.experimental import pallas as pl
from jax.experimental.pallas import tpu as pltpu
from jax.sharding import PartitionSpec as P

MESH = pl.DeviceIdType.MESH
F32, BF16 = jnp.float32, jnp.bfloat16
EXACT = lax.Precision.HIGHEST


def up(value, step):
    return -(-value // step) * step


def dot(a, b, ca, cb, precision=None):
    return lax.dot_general(
        a, b, (((ca,), (cb,)), ((), ())), preferred_element_type=F32, precision=precision
    )


def when(condition, run):
    if condition is True:
        run()
    else:
        pl.when(condition)(run)


def lower_inverse(gram, size, look=4):
    full = gram.shape[0]
    lane = lax.broadcasted_iota(jnp.int32, (1, full), 1)
    top, table, done = 0, gram, []
    for first in range(0, size, look):
        base = first // 8 * 8
        if base > top:
            done.append(table[: base - top])
            table = table[base - top :]
            top = base
        rows = full - top
        width = min(look, size - first)
        row_id = lax.broadcasted_iota(jnp.int32, (rows, full), 0) + top
        columns = [
            jnp.broadcast_to(table[:, first + t : first + t + 1], (rows, full)) for t in range(width)
        ]
        for t in range(width):
            j = first + t
            here = j - top
            column = columns[t]
            pivot = column[here : here + 1]
            inverse = 1.0 / pivot
            row = jnp.where(lane == j, 1.0, table[here : here + 1]) * inverse
            below = row_id > j
            lower = jnp.where(below, column, 0.0)
            for s in range(t + 1, width):
                ahead = here + s - t
                columns[s] = columns[s] - lower * (column[ahead : ahead + 1] * inverse)
            table = jnp.where((lane == j) & below, 0.0, table) - lower * row
    done.append(table)
    table = jnp.concatenate(done, axis=0) if len(done) > 1 else table
    row_id = lax.broadcasted_iota(jnp.int32, (full, full), 0)
    lane = lax.broadcasted_iota(jnp.int32, (full, full), 1)
    pivots = jnp.sum(jnp.where(row_id == lane, table, 0.0), axis=1, keepdims=True)
    unit = jnp.where(row_id > lane, table, jnp.where(row_id == lane, 1.0, 0.0))
    return unit * lax.rsqrt(pivots)


def kernel(
    dims,
    core_ref,
    gauss_ref,
    left_ref,
    right_ref,
    frames_ref,
    faces_ref,
    sketch_buf,
    part_out,
    part_in,
    carry_buf,
    carry_own,
    proj_out,
    proj_in,
    gram_out,
    gram_in,
    piece_sk,
    piece_ca,
    s_part,
    r_part,
    s_sk,
    r_sk,
    s_proj,
    r_proj,
    s_gram,
    r_gram,
    s_next,
    r_next,
    s_own,
    r_own,
):
    size, group_count, rank, sketch, modes, chunk, owners, scale = dims
    rank_pad, sketch_pad = sketch_buf.shape
    me = lax.axis_index("mode")
    group = lax.axis_index("cores")
    final = group_count - 1
    owner = True if owners == size else me < owners
    down = lax.rem(group + group_count - 1, group_count)
    upward = lax.rem(group + 1, group_count)

    barrier = pltpu.get_barrier_semaphore()

    def greet(to_group, first):
        for d in range(first, size):
            pl.semaphore_signal(
                barrier,
                inc=1,
                device_id={"mode": lax.rem(me + d, size), "cores": to_group},
                device_id_type=MESH,
            )

    greet(group, 1)
    pl.when(group < final)(lambda: greet(upward, 0))
    pl.when(group > 0)(lambda: greet(down, 0))

    @pl.when(group == 0)
    def _():
        pl.semaphore_wait(barrier, 2 * size - 1)

    @pl.when((group > 0) & (group < final))
    def _():
        pl.semaphore_wait(barrier, 3 * size - 1)

    def block(ref, index):
        return ref.at[pl.ds(pl.multiple_of(index * chunk, chunk), chunk)]

    def scatter(out_ref, in_ref, sends, recvs, whole=False):
        copies = []
        for d in range(1, size):
            peer = lax.rem(me + d, size)
            copies.append(
                pltpu.make_async_remote_copy(
                    src_ref=out_ref if whole else block(out_ref, peer),
                    dst_ref=in_ref.at[d],
                    send_sem=sends.at[d],
                    recv_sem=recvs.at[d],
                    device_id={"mode": peer},
                    device_id_type=MESH,
                )
            )
        return copies

    def chunk_sends(copies, act):
        for d, copy in enumerate(copies, 1):
            peer = lax.rem(me + d, size)
            when(True if owners == size else peer < owners, functools.partial(act, copy))

    def spread(piece_ref, buf_ref, sends, recvs, to_group, first):
        copies = []
        for d in range(first, size):
            peer = lax.rem(me + d, size)
            copies.append(
                pltpu.make_async_remote_copy(
                    src_ref=piece_ref,
                    dst_ref=block(buf_ref, me),
                    send_sem=sends.at[d],
                    recv_sem=recvs.at[me],
                    device_id={"mode": peer, "cores": to_group},
                    device_id_type=MESH,
                )
            )
        return copies

    def await_chunk(buf_ref, recvs, source):
        pltpu.make_async_remote_copy(
            src_ref=block(buf_ref, source),
            dst_ref=block(buf_ref, source),
            send_sem=recvs.at[source],
            recv_sem=recvs.at[source],
            device_id={"mode": lax.rem(me + 1, size)},
            device_id_type=MESH,
        ).wait_recv()

    if rank_pad > rank:
        rest = jnp.zeros((rank_pad - rank, sketch_pad), F32)
        part_out[pl.ds(rank, rank_pad - rank), :] = rest.astype(part_out.dtype)
        proj_out[pl.ds(rank, rank_pad - rank), :] = rest

    @pl.when(group == final)
    def _():
        sketch_buf[...] = right_ref[...]

    @pl.when(group < final)
    def _():
        for source in range(owners):
            await_chunk(sketch_buf, r_sk, source)

    part_copies = scatter(part_out, part_in, s_part, r_part)
    sk_copies = spread(piece_sk, sketch_buf, s_sk, r_sk, down, 0)
    held = sketch_buf[pl.ds(0, rank), :]
    partials = [dot(core_ref[i], held, 1, 0).astype(BF16) for i in range(modes)]

    @pl.when(group > 0)
    def _():
        total = None
        for i in range(modes):
            term = dot(partials[i], gauss_ref[i], 1, 1)
            total = term if total is None else total + term
        part_out[pl.ds(0, rank), :] = total.astype(part_out.dtype)

        @pl.when(group == final)
        def _():
            pl.semaphore_wait(barrier, 2 * size - 1)

        chunk_sends(part_copies, lambda c: c.start())

        def finish():
            value = block(part_out, me)[...].astype(F32)
            for d in range(1, size):
                part_copies[d - 1].wait_recv()
                value = value + part_in[d].astype(F32)
            piece_sk[...] = value.astype(BF16)
            for copy in sk_copies:
                copy.start()
            for copy in sk_copies:
                copy.wait_send()

        when(owner, finish)
        chunk_sends(part_copies, lambda c: c.wait_send())

    @pl.when(group == 0)
    def _():
        carry_buf[...] = left_ref[...]

    @pl.when(group > 0)
    def _():
        for source in range(owners):
            await_chunk(carry_buf, r_next, source)

    carry = carry_buf[pl.ds(0, rank), :].T
    gram_copies = scatter(gram_out, gram_in, s_gram, r_gram, True)
    proj_copies = scatter(proj_out, proj_in, s_proj, r_proj)
    images = [dot(carry, partials[i], 1, 0) for i in range(modes)]
    image = jnp.concatenate(images, axis=0)
    high = image.astype(BF16)
    low = (image - high.astype(F32)).astype(BF16)
    pair = jnp.concatenate([high, low], axis=1)
    terms = dot(high, pair, 0, 0)
    cross = terms[:, sketch_pad:]
    gram = terms[:, :sketch_pad] + cross + cross.T
    gram_rows = gram_out.shape[0]
    gram_out[...] = gram[:gram_rows]
    for copy in gram_copies:
        copy.start()
    built = jnp.concatenate(
        [dot(carry, core_ref[i], 1, 0).astype(BF16) for i in range(modes)], axis=0
    )
    proj = dot(built, pair, 0, 0)
    proj_out[pl.ds(0, rank), :] = proj[:, :sketch_pad] + proj[:, sketch_pad:]
    chunk_sends(proj_copies, lambda c: c.start())

    gram_in[0] = gram_out[...]
    for copy in gram_copies:
        copy.wait_recv()
    total = None
    for source in range(size):
        term = gram_in[lax.rem(me - source + size, size)]
        total = term if total is None else total + term
    if gram_rows < sketch_pad:
        total = jnp.concatenate([total, jnp.zeros((sketch_pad - gram_rows, sketch_pad), F32)], 0)
    row_id = lax.broadcasted_iota(jnp.int32, (sketch_pad, sketch_pad), 0)
    lane_id = lax.broadcasted_iota(jnp.int32, (sketch_pad, sketch_pad), 1)
    total = jnp.where((row_id == lane_id) & (row_id >= sketch), 1.0, total)
    inverse = lower_inverse(total, sketch, 8)

    next_copies = spread(piece_ca, carry_buf, s_next, r_next, upward, 0)
    own_copies = spread(piece_ca, carry_own, s_own, r_own, group, 1)

    def project():
        value = block(proj_out, me)[...]
        for d in range(1, size):
            proj_copies[d - 1].wait_recv()
            value = value + proj_in[d]
        piece_ca[...] = dot(value, inverse, 1, 1, EXACT).astype(BF16)

        @pl.when(group < final)
        def _():
            for copy in next_copies:
                copy.start()

        for copy in own_copies:
            copy.start()
        block(carry_own, me)[...] = piece_ca[...]

    when(owner, project)
    orth = (dot(image, inverse, 1, 1, EXACT) * scale).astype(BF16)
    for i in range(modes):
        frames_ref[i] = orth[i * sketch_pad : (i + 1) * sketch_pad]
    chunk_sends(proj_copies, lambda c: c.wait_send())
    for copy in gram_copies:
        copy.wait_send()
    for source in range(owners):

        @pl.when(me != source)
        def _(source=source):
            await_chunk(carry_own, r_own, source)

    faces_ref[...] = carry_own[...].T.astype(F32)

    def drain():
        for copy in own_copies:
            copy.wait_send()

        @pl.when(group < final)
        def _():
            for copy in next_copies:
                copy.wait_send()

    when(owner, drain)


def body(train_cores, sketch_cores, left_interface, right_sketch):
    size = lax.axis_size("mode")
    group_count = lax.axis_size("cores")
    _, rank, modes, _ = train_cores.shape
    sketch = sketch_cores.shape[1]
    sketch_pad = up(sketch, 128)
    chunk = up(-(-up(rank, 128) // size), 16)
    owners = -(-rank // chunk)
    rank_pad = owners * chunk
    core = train_cores[0].transpose(1, 0, 2)
    gauss = jnp.pad(
        sketch_cores[0].transpose(1, 0, 2),
        ((0, 0), (0, sketch_pad - sketch), (0, sketch_pad - sketch)),
    )
    sides = ((0, rank_pad - rank), (0, sketch_pad - sketch))
    left = jnp.pad(left_interface.astype(BF16).T, sides)
    right = jnp.pad(right_sketch, sides)
    scale = math.sqrt(sketch * modes * size)
    dims = (size, group_count, rank, sketch, modes, chunk, owners, scale)
    gram_rows = up(sketch, 8)
    chunks = (rank_pad, sketch_pad)
    vmem = pl.BlockSpec(memory_space=pltpu.VMEM)
    dma = pltpu.SemaphoreType.DMA((size,))
    frames, faces = pl.pallas_call(
        functools.partial(kernel, dims),
        out_shape=(
            jax.ShapeDtypeStruct((modes, sketch_pad, sketch_pad), BF16),
            jax.ShapeDtypeStruct((sketch_pad, rank_pad), F32),
        ),
        in_specs=[vmem] * 4,
        out_specs=(vmem, vmem),
        scratch_shapes=[
            pltpu.VMEM(chunks, BF16),
            pltpu.VMEM((size * chunk, sketch_pad), BF16),
            pltpu.VMEM((size, chunk, sketch_pad), BF16),
            pltpu.VMEM(chunks, BF16),
            pltpu.VMEM(chunks, BF16),
            pltpu.VMEM((size * chunk, sketch_pad), F32),
            pltpu.VMEM((size, chunk, sketch_pad), F32),
            pltpu.VMEM((gram_rows, sketch_pad), F32),
            pltpu.VMEM((size, gram_rows, sketch_pad), F32),
            pltpu.VMEM((chunk, sketch_pad), BF16),
            pltpu.VMEM((chunk, sketch_pad), BF16),
        ]
        + [dma] * 12,
        compiler_params=pltpu.CompilerParams(collective_id=0, has_side_effects=True),
    )(core, gauss, left, right)
    frames = frames[:, :sketch, :sketch].transpose(1, 0, 2)[None]
    return frames, faces[None, :sketch, :rank]


def solution(mesh):
    in_specs = (P("cores", None, "mode", None), P("cores", None, "mode", None), P(), P())
    out_specs = (P("cores", None, "mode", None), P("cores", None, None))
    return jax.shard_map(body, mesh=mesh, in_specs=in_specs, out_specs=out_specs, check_vma=False)
```

```python
import functools
import math

import jax
import jax.numpy as jnp
from jax import lax
from jax.experimental import pallas as pl
from jax.experimental.pallas import tpu as pltpu
from jax.sharding import PartitionSpec as P

MESH = pl.DeviceIdType.MESH
F32, BF16 = jnp.float32, jnp.bfloat16
EXACT = lax.Precision.HIGHEST


def up(value, step):
    return -(-value // step) * step


def dot(a, b, ca, cb, precision=None):
    return lax.dot_general(
        a, b, (((ca,), (cb,)), ((), ())), preferred_element_type=F32, precision=precision
    )


def when(condition, run):
    if condition is True:
        run()
    else:
        pl.when(condition)(run)


def lower_inverse(gram, size, look=4):
    full = gram.shape[0]
    lane = lax.broadcasted_iota(jnp.int32, (1, full), 1)
    top, table, done = 0, gram, []
    for first in range(0, size, look):
        base = first // 8 * 8
        if base > top:
            done.append(table[: base - top])
            table = table[base - top :]
            top = base
        rows = full - top
        width = min(look, size - first)
        row_id = lax.broadcasted_iota(jnp.int32, (rows, full), 0) + top
        columns = [
            jnp.broadcast_to(table[:, first + t : first + t + 1], (rows, full)) for t in range(width)
        ]
        for t in range(width):
            j = first + t
            here = j - top
            column = columns[t]
            pivot = column[here : here + 1]
            inverse = 1.0 / pivot
            row = jnp.where(lane == j, 1.0, table[here : here + 1]) * inverse
            below = row_id > j
            lower = jnp.where(below, column, 0.0)
            for s in range(t + 1, width):
                ahead = here + s - t
                columns[s] = columns[s] - lower * (column[ahead : ahead + 1] * inverse)
            table = jnp.where((lane == j) & below, 0.0, table) - lower * row
    done.append(table)
    table = jnp.concatenate(done, axis=0) if len(done) > 1 else table
    row_id = lax.broadcasted_iota(jnp.int32, (full, full), 0)
    lane = lax.broadcasted_iota(jnp.int32, (full, full), 1)
    pivots = jnp.sum(jnp.where(row_id == lane, table, 0.0), axis=1, keepdims=True)
    unit = jnp.where(row_id > lane, table, jnp.where(row_id == lane, 1.0, 0.0))
    return unit * lax.rsqrt(pivots)


def kernel(
    dims,
    core_ref,
    gauss_ref,
    left_ref,
    right_ref,
    frames_ref,
    faces_ref,
    sketch_buf,
    part_out,
    part_in,
    carry_buf,
    carry_own,
    proj_out,
    proj_in,
    gram_out,
    gram_in,
    piece_sk,
    piece_ca,
    s_part,
    r_part,
    s_sk,
    r_sk,
    s_proj,
    r_proj,
    s_gram,
    r_gram,
    s_next,
    r_next,
    s_own,
    r_own,
):
    size, group_count, rank, sketch, modes, chunk, owners, scale = dims
    rank_pad, sketch_pad = sketch_buf.shape
    me = lax.axis_index("mode")
    group = lax.axis_index("cores")
    final = group_count - 1
    owner = True if owners == size else me < owners
    down = lax.rem(group + group_count - 1, group_count)
    upward = lax.rem(group + 1, group_count)

    barrier = pltpu.get_barrier_semaphore()

    def greet(to_group, first):
        for d in range(first, size):
            pl.semaphore_signal(
                barrier,
                inc=1,
                device_id={"mode": lax.rem(me + d, size), "cores": to_group},
                device_id_type=MESH,
            )

    greet(group, 1)
    pl.when(group < final)(lambda: greet(upward, 0))
    pl.when(group > 0)(lambda: greet(down, 0))

    @pl.when(group == 0)
    def _():
        pl.semaphore_wait(barrier, 2 * size - 1)

    @pl.when((group > 0) & (group < final))
    def _():
        pl.semaphore_wait(barrier, 3 * size - 1)

    def block(ref, index):
        return ref.at[pl.ds(pl.multiple_of(index * chunk, chunk), chunk)]

    def scatter(out_ref, in_ref, sends, recvs, whole=False):
        copies = []
        for d in range(1, size):
            peer = lax.rem(me + d, size)
            copies.append(
                pltpu.make_async_remote_copy(
                    src_ref=out_ref if whole else block(out_ref, peer),
                    dst_ref=in_ref.at[d],
                    send_sem=sends.at[d],
                    recv_sem=recvs.at[d],
                    device_id={"mode": peer},
                    device_id_type=MESH,
                )
            )
        return copies

    def chunk_sends(copies, act):
        for d, copy in enumerate(copies, 1):
            peer = lax.rem(me + d, size)
            when(True if owners == size else peer < owners, functools.partial(act, copy))

    def spread(piece_ref, buf_ref, sends, recvs, to_group, first):
        copies = []
        for d in range(first, size):
            peer = lax.rem(me + d, size)
            copies.append(
                pltpu.make_async_remote_copy(
                    src_ref=piece_ref,
                    dst_ref=block(buf_ref, me),
                    send_sem=sends.at[d],
                    recv_sem=recvs.at[me],
                    device_id={"mode": peer, "cores": to_group},
                    device_id_type=MESH,
                )
            )
        return copies

    def await_chunk(buf_ref, recvs, source):
        pltpu.make_async_remote_copy(
            src_ref=block(buf_ref, source),
            dst_ref=block(buf_ref, source),
            send_sem=recvs.at[source],
            recv_sem=recvs.at[source],
            device_id={"mode": lax.rem(me + 1, size)},
            device_id_type=MESH,
        ).wait_recv()

    if rank_pad > rank:
        proj_out[pl.ds(rank, rank_pad - rank), :] = jnp.zeros((rank_pad - rank, sketch_pad), F32)
    part_out[...] = jnp.zeros(part_out.shape, part_out.dtype)

    @pl.when(group == final)
    def _():
        sketch_buf[...] = jnp.zeros(sketch_buf.shape, BF16)
        sketch_buf[pl.ds(0, rank), pl.ds(0, sketch)] = right_ref[...]

    @pl.when(group < final)
    def _():
        for source in range(owners):
            await_chunk(sketch_buf, r_sk, source)

    part_copies = scatter(part_out, part_in, s_part, r_part)
    sk_copies = spread(piece_sk, sketch_buf, s_sk, r_sk, down, 0)
    held = sketch_buf[pl.ds(0, rank), :]
    partials = [dot(core_ref[i], held, 1, 0).astype(BF16) for i in range(modes)]

    @pl.when(group > 0)
    def _():
        total = None
        for i in range(modes):
            term = dot(partials[i][:, :sketch], gauss_ref[i], 1, 1)
            total = term if total is None else total + term
        part_out[pl.ds(0, rank), pl.ds(0, sketch)] = total.astype(part_out.dtype)

        @pl.when(group == final)
        def _():
            pl.semaphore_wait(barrier, 2 * size - 1)

        chunk_sends(part_copies, lambda c: c.start())

        def finish():
            value = block(part_out, me)[...].astype(F32)
            for d in range(1, size):
                part_copies[d - 1].wait_recv()
                value = value + part_in[d].astype(F32)
            piece_sk[...] = value.astype(BF16)
            for copy in sk_copies:
                copy.start()
            for copy in sk_copies:
                copy.wait_send()

        when(owner, finish)
        chunk_sends(part_copies, lambda c: c.wait_send())

    @pl.when(group == 0)
    def _():
        carry_buf[...] = jnp.zeros(carry_buf.shape, BF16)
        carry_buf[pl.ds(0, rank), pl.ds(0, sketch)] = left_ref[...].T.astype(BF16)

    @pl.when(group > 0)
    def _():
        for source in range(owners):
            await_chunk(carry_buf, r_next, source)

    carry = carry_buf[pl.ds(0, rank), :].T
    gram_copies = scatter(gram_out, gram_in, s_gram, r_gram, True)
    proj_copies = scatter(proj_out, proj_in, s_proj, r_proj)
    images = [dot(carry, partials[i], 1, 0) for i in range(modes)]
    image = jnp.concatenate(images, axis=0)
    high = image.astype(BF16)
    low = (image - high.astype(F32)).astype(BF16)
    pair = jnp.concatenate([high, low], axis=1)
    terms = dot(high, pair, 0, 0)
    cross = terms[:, sketch_pad:]
    gram = terms[:, :sketch_pad] + cross + cross.T
    half, quarter = sketch_pad // 2, sketch_pad // 4
    lower_rows = gram_out.shape[0] - quarter
    gram_out[pl.ds(0, lower_rows), :] = gram[half : half + lower_rows]
    gram_out[pl.ds(lower_rows, quarter), :] = jnp.concatenate(
        [gram[:quarter, :half], gram[quarter:half, :half]], axis=1
    )
    for copy in gram_copies:
        copy.start()
    built = jnp.concatenate(
        [dot(carry, core_ref[i], 1, 0).astype(BF16) for i in range(modes)], axis=0
    )
    proj = dot(built, pair, 0, 0)
    proj_out[pl.ds(0, rank), :] = proj[:, :sketch_pad] + proj[:, sketch_pad:]
    chunk_sends(proj_copies, lambda c: c.start())

    gram_in[0] = gram_out[...]
    for copy in gram_copies:
        copy.wait_recv()
    total = None
    for source in range(size):
        term = gram_in[lax.rem(me - source + size, size)]
        total = term if total is None else total + term
    lower = total[:lower_rows]
    if lower_rows < half:
        lower = jnp.concatenate([lower, jnp.zeros((half - lower_rows, sketch_pad), F32)], axis=0)
    corner = total[lower_rows:]
    corner = jnp.concatenate([corner[:, :half], corner[:, half:]], axis=0)
    upper = jnp.concatenate([corner, lower.T[:half]], axis=1)
    total = jnp.concatenate([upper, lower], axis=0)
    row_id = lax.broadcasted_iota(jnp.int32, (sketch_pad, sketch_pad), 0)
    lane_id = lax.broadcasted_iota(jnp.int32, (sketch_pad, sketch_pad), 1)
    total = jnp.where((row_id == lane_id) & (row_id >= sketch), 1.0, total)
    inverse = lower_inverse(total, sketch, 8)

    next_copies = spread(piece_ca, carry_buf, s_next, r_next, upward, 0)
    own_copies = spread(piece_ca, carry_own, s_own, r_own, group, 1)

    def project():
        value = block(proj_out, me)[...]
        for d in range(1, size):
            proj_copies[d - 1].wait_recv()
            value = value + proj_in[d]
        piece_ca[...] = dot(value, inverse, 1, 1, EXACT).astype(BF16)

        @pl.when(group < final)
        def _():
            for copy in next_copies:
                copy.start()

        for copy in own_copies:
            copy.start()
        block(carry_own, me)[...] = piece_ca[...]

    when(owner, project)
    orth = (dot(image, inverse, 1, 1, EXACT) * scale).astype(BF16)
    for i in range(modes):
        frames_ref[i] = orth[i * sketch_pad : (i + 1) * sketch_pad]
    chunk_sends(proj_copies, lambda c: c.wait_send())
    for copy in gram_copies:
        copy.wait_send()
    for source in range(owners):

        @pl.when(me != source)
        def _(source=source):
            await_chunk(carry_own, r_own, source)

    faces_ref[...] = carry_own[...].T.astype(F32)

    def drain():
        for copy in own_copies:
            copy.wait_send()

        @pl.when(group < final)
        def _():
            for copy in next_copies:
                copy.wait_send()

    when(owner, drain)


def body(train_cores, sketch_cores, left_interface, right_sketch):
    size = lax.axis_size("mode")
    group_count = lax.axis_size("cores")
    _, rank, modes, _ = train_cores.shape
    sketch = sketch_cores.shape[1]
    sketch_pad = up(sketch, 128)
    chunk = up(-(-up(rank, 128) // size), 16)
    owners = -(-rank // chunk)
    rank_pad = owners * chunk
    core = train_cores[0].transpose(1, 0, 2)
    gauss = sketch_cores[0].transpose(1, 0, 2)
    scale = math.sqrt(sketch * modes * size)
    dims = (size, group_count, rank, sketch, modes, chunk, owners, scale)
    gram_rows = up(max(sketch - sketch_pad // 2, 8), 8) + sketch_pad // 4
    chunks = (rank_pad, sketch_pad)
    vmem = pl.BlockSpec(memory_space=pltpu.VMEM)
    dma = pltpu.SemaphoreType.DMA((size,))
    frames, faces = pl.pallas_call(
        functools.partial(kernel, dims),
        out_shape=(
            jax.ShapeDtypeStruct((modes, sketch_pad, sketch_pad), BF16),
            jax.ShapeDtypeStruct((sketch_pad, rank_pad), F32),
        ),
        in_specs=[vmem] * 4,
        out_specs=(vmem, vmem),
        scratch_shapes=[
            pltpu.VMEM(chunks, BF16),
            pltpu.VMEM((size * chunk, sketch_pad), BF16),
            pltpu.VMEM((size, chunk, sketch_pad), BF16),
            pltpu.VMEM(chunks, BF16),
            pltpu.VMEM(chunks, BF16),
            pltpu.VMEM((size * chunk, sketch_pad), F32),
            pltpu.VMEM((size, chunk, sketch_pad), F32),
            pltpu.VMEM((gram_rows, sketch_pad), F32),
            pltpu.VMEM((size, gram_rows, sketch_pad), F32),
            pltpu.VMEM((chunk, sketch_pad), BF16),
            pltpu.VMEM((chunk, sketch_pad), BF16),
        ]
        + [dma] * 12,
        compiler_params=pltpu.CompilerParams(collective_id=0, has_side_effects=True),
    )(core, gauss, left_interface, right_sketch)
    frames = frames[:, :sketch, :sketch].transpose(1, 0, 2)[None]
    return frames, faces[None, :sketch, :rank]


def solution(mesh):
    in_specs = (P("cores", None, "mode", None), P("cores", None, "mode", None), P(), P())
    out_specs = (P("cores", None, "mode", None), P("cores", None, None))
    return jax.shard_map(body, mesh=mesh, in_specs=in_specs, out_specs=out_specs, check_vma=False)
```
